32 devices in a mesh: stage: 1 (over z), fsdp: 4 (over y), tp: 8 (over x, core).
Axes of the slice: x: 4, y: 4, z: 1, core: 2. Of those that a mesh axis runs over, the one named last changes fastest.
The devices are a block of a 4x4x8 slice.
Arguments:
- weight: float32 [4, 1536, 12288], P('stage', 'fsdp', 'tp')
- momentum: float32 [4, 1536, 12288], P('stage', 'fsdp', 'tp')
- gradient: bfloat16 [4, 1536, 12288], P('stage', 'fsdp', 'tp')
- learn_rate: float32 [], replicated
- momentum_coef: float32 [], replicated
- weight_decay: float32 [], replicated
Outputs:
- output 1: float32 [4, 1536, 12288], P('stage', 'fsdp', 'tp')
- output 2: float32 [4, 1536, 12288], P('stage', 'fsdp', 'tp')
All inputs are finite; a program needn't handle non-finite values.
Results may differ from the reference program's by a relative error of at most 0.0156467.
Values are sent between devices in bfloat16 or wider.
A program may use at most 768 MiB of HBM per device.

```python
import math
import jax
import jax.numpy as jnp
from jax import lax

LAYERS = 4
D_ROW = 1536
D_COL = 12288
RANK = 16
NS_STEPS = 5
COEF_A = 3.4445
COEF_B = -4.7750
COEF_C = 2.0315
EPSILON = 1e-7


def draw_matrix(key):
    k_left, k_right, k_noise = jax.random.split(key, 3)
    left = jax.random.normal(k_left, (LAYERS, D_ROW, RANK), jnp.float32)
    right = jax.random.normal(k_right, (LAYERS, RANK, D_COL), jnp.float32)
    noise = jax.random.normal(k_noise, (LAYERS, D_ROW, D_COL), jnp.float32)
    return 0.25 * (jnp.einsum('lrk,lkc->lrc', left, right) * (RANK ** -0.5) + 0.5 * noise)


def setup_inputs(seed: int = 0, part: int = 0) -> dict:
    part_key = jax.random.fold_in(jax.random.key(seed), part)
    k_weight, k_mom, k_grad = jax.random.split(part_key, 3)
    k_rate, k_coef, k_decay = jax.random.split(jax.random.key(seed + 1), 3)
    weight = jax.random.normal(k_weight, (LAYERS, D_ROW, D_COL), jnp.float32)
    momentum = draw_matrix(k_mom)
    gradient = draw_matrix(k_grad).astype(jnp.bfloat16)
    learn_rate = jax.random.uniform(k_rate, (), jnp.float32, 0.25, 2.0)
    momentum_coef = jax.random.uniform(k_coef, (), jnp.float32, 0.4, 0.95)
    weight_decay = jax.random.uniform(k_decay, (), jnp.float32, 0.05, 0.45)
    return {'weight': weight, 'momentum': momentum, 'gradient': gradient, 'learn_rate': learn_rate, 'momentum_coef': momentum_coef, 'weight_decay': weight_decay}


def orthogonalize(x_init):
    frob_norm = jnp.sqrt(jnp.sum(x_init * x_init))
    x_start = (x_init / (frob_norm + EPSILON)).astype(jnp.bfloat16)

    def ns_step(x_cur, unused):
        gram_mat = jnp.dot(x_cur, x_cur.T, preferred_element_type=jnp.float32).astype(jnp.bfloat16)
        gram_sq = jnp.dot(gram_mat, gram_mat, preferred_element_type=jnp.float32).astype(jnp.bfloat16)
        poly_mat = (COEF_B * gram_mat.astype(jnp.float32) + COEF_C * gram_sq.astype(jnp.float32)).astype(jnp.bfloat16)
        poly_x = jnp.dot(poly_mat, x_cur, preferred_element_type=jnp.float32)
        x_next = (COEF_A * x_cur.astype(jnp.float32) + poly_x).astype(jnp.bfloat16)
        return x_next, None

    x_out, _ = lax.scan(ns_step, x_start, None, length=NS_STEPS)
    return x_out


def reference(weight, momentum, gradient, learn_rate, momentum_coef, weight_decay):
    step_scale = learn_rate * 0.2 * math.sqrt(D_COL)
    keep_scale = 1.0 - learn_rate * weight_decay

    def one_matrix(blocks):
        w_mat, m_mat, g_mat = blocks
        g_wide = g_mat.astype(jnp.float32)
        m_new = momentum_coef * m_mat + g_wide
        x_init = g_wide + momentum_coef * m_new
        x_orth = orthogonalize(x_init)
        w_new = keep_scale * w_mat - step_scale * x_orth.astype(jnp.float32)
        return w_new, m_new

    new_weight, new_momentum = lax.map(one_matrix, (weight, momentum, gradient))
    return new_weight, new_momentum
```

```python
import math
import jax
import jax.numpy as jnp
from jax import lax
from jax.sharding import PartitionSpec as P

NS_STEPS = 5
COEF_A = 3.4445
COEF_B = -4.7750
COEF_C = 2.0315
EPSILON = 1e-7
F32 = jnp.float32
BF16 = jnp.bfloat16


def solution(mesh):
    block_spec = P('stage', 'fsdp', 'tp')
    scalar_spec = P()

    def muon_step(weight, momentum, gradient, learn_rate, momentum_coef, weight_decay):
        n_cols = weight.shape[2]

        def local_step(w_blk, m_blk, g_blk, rate_val, coef_val, decay_val):
            g_wide = g_blk.astype(F32)
            m_new = coef_val * m_blk + g_wide
            x_init = g_wide + coef_val * m_new
            sq_sum = lax.psum(jnp.sum(x_init * x_init, axis=(1, 2), keepdims=True), ('fsdp', 'tp'))
            x_home = (x_init / (jnp.sqrt(sq_sum) + EPSILON)).astype(BF16)
            x = lax.all_to_all(x_home, 'fsdp', split_axis=0, concat_axis=1, tiled=True)
            for _ in range(NS_STEPS):
                part = jnp.einsum('lrk,lsk->lrs', x, x, preferred_element_type=F32)
                mine = lax.psum_scatter(part, 'tp', scatter_dimension=1, tiled=True).astype(BF16)
                gram = lax.all_gather(mine, 'tp', axis=1, tiled=True)
                sq = jnp.einsum('lrk,lks->lrs', gram, gram, preferred_element_type=F32).astype(BF16)
                poly = (COEF_B * gram.astype(F32) + COEF_C * sq.astype(F32)).astype(BF16)
                px = jnp.einsum('lrk,lkc->lrc', poly, x, preferred_element_type=F32)
                x = (COEF_A * x.astype(F32) + px).astype(BF16)
            x_home = lax.all_to_all(x, 'fsdp', split_axis=1, concat_axis=0, tiled=True)
            step_scale = rate_val * 0.2 * math.sqrt(n_cols)
            keep_scale = 1.0 - rate_val * decay_val
            w_new = keep_scale * w_blk - step_scale * x_home.astype(F32)
            return w_new, m_new

        sharded = jax.shard_map(local_step, mesh=mesh, in_specs=(block_spec, block_spec, block_spec, scalar_spec, scalar_spec, scalar_spec), out_specs=(block_spec, block_spec), check_vma=False)
        return sharded(weight, momentum, gradient, learn_rate, momentum_coef, weight_decay)

    return muon_step
```

```python
import functools
import math

import jax
import jax.numpy as jnp
from jax import lax
from jax.experimental import pallas as pl
from jax.experimental.pallas import tpu as pltpu
from jax.sharding import PartitionSpec as P

NS_STEPS = 5
COEF_A = 3.4445
COEF_B = -4.7750
COEF_C = 2.0315
EPSILON = 1e-7
F32 = jnp.float32
BF16 = jnp.bfloat16
MESH = pl.DeviceIdType.MESH
N_STRIP = 4
N_SUB = 2
NT = (((1,), (1,)), ((), ()))


def muon_kernel(strip, cols, sq_ref, x0_hbm, out_hbm,
                x0, xs, relay_in, relay_out, x, part, pair, ring, packed, gram, poly, nrm_y, nrm_x, nrm_c, nrm,
                x0_sem, own_sem, nrm_s, nrm_r, a2a_s, a2a_r, ret_s, ret_r,
                pair_s, pair_r, rs_s, rs_r, ag_s, ag_r, pg_s, pg_r, poly_s, poly_r):
    f = lax.axis_index('fsdp')
    tp = lax.axis_index('tp')
    chip, core = tp // 2, tp % 2
    sub3 = strip // 3
    half_rows = (2 * sub3 + strip + strip // 2) // 2
    piece = half_rows // N_SUB
    hop = 1 - 2 * core

    def wrap(i):
        return lax.rem(i + 2 * N_STRIP, N_STRIP)

    def y_dev(k):
        return {'fsdp': wrap(f + k)}

    def x_dev(k):
        return {'tp': 2 * wrap(chip + k) + core}

    partner = {'tp': 2 * chip + (1 - core)}
    ahead = x_dev(hop)

    def send(src, dst, s_sem, r_sem, dev):
        copy = pltpu.make_async_remote_copy(src_ref=src, dst_ref=dst, send_sem=s_sem, recv_sem=r_sem,
                                            device_id=dev, device_id_type=MESH)
        copy.start()
        return copy

    loads = [pltpu.make_async_copy(x0_hbm.at[i], x0.at[i], x0_sem.at[i]) for i in range(N_STRIP)]
    for c in loads:
        c.start()

    barrier = pltpu.get_barrier_semaphore()
    for dev in [y_dev(1), y_dev(2), y_dev(3), x_dev(1), x_dev(2), x_dev(3), partner]:
        pl.semaphore_signal(barrier, inc=1, device_id=dev, device_id_type=MESH)
    pl.semaphore_wait(barrier, 7)

    nrm_y[f] = sq_ref[...]
    cs = [send(sq_ref, nrm_y.at[f], nrm_s.at[k - 1], nrm_r.at[k - 1], y_dev(k)) for k in (1, 2, 3)]
    for c in cs:
        c.wait()
    nrm_x[chip] = (nrm_y[0] + nrm_y[1]) + (nrm_y[2] + nrm_y[3])
    cs = [send(nrm_x.at[chip], nrm_x.at[chip], nrm_s.at[k + 2], nrm_r.at[k + 2], x_dev(k)) for k in (1, 2, 3)]
    for c in cs:
        c.wait()
    nrm_c[core] = (nrm_x[0] + nrm_x[1]) + (nrm_x[2] + nrm_x[3])
    send(nrm_c.at[core], nrm_c.at[core], nrm_s.at[6], nrm_r.at[6], partner).wait()
    nrm[...] = 1.0 / (jnp.sqrt(nrm_c[0] + nrm_c[1]) + EPSILON)
    for c in loads:
        c.wait()

    tile = strip // 6
    h = strip // 2

    def scale_to(i, dst, base):
        inv = nrm[pl.ds(i, 1), :][:, 0:1]

        @pl.loop(0, strip // tile)
        def _(r):
            rows = pl.ds(pl.multiple_of(r * tile, tile), tile)
            dst[pl.ds(pl.multiple_of(base + r * tile, tile), tile), :] = (x0[i, rows, :] * inv).astype(BF16)

    def exchange(src, dst, relay, s_sem, r_sem, make):
        make(2)
        r0 = send(src(2).at[pl.ds(0, h)], relay.at[0], s_sem.at[0], r_sem.at[0], y_dev(1))
        r1 = send(src(2).at[pl.ds(h, h)], relay.at[1], s_sem.at[1], r_sem.at[1], y_dev(-1))
        make(1)
        d0 = send(src(1), dst(0), s_sem.at[2], r_sem.at[2], y_dev(1))
        make(-1)
        d1 = send(src(-1), dst(0), s_sem.at[3], r_sem.at[3], y_dev(-1))
        make(0)
        r0.wait_recv()
        f0 = send(relay.at[0], dst(-1).at[pl.ds(0, h)], s_sem.at[4], r_sem.at[4], y_dev(1))
        r1.wait_recv()
        f1 = send(relay.at[1], dst(1).at[pl.ds(h, h)], s_sem.at[5], r_sem.at[5], y_dev(-1))
        r0.wait_send()
        r1.wait_send()
        for c in (d0, d1, f0, f1):
            c.wait()

    def strip_of(ref, i):
        return ref.at[pl.ds(pl.multiple_of(i * strip, strip), strip)]

    def make_in(k):
        i = wrap(f + k)
        if k == 0:
            scale_to(i, x.at[0], i * strip)
        else:
            scale_to(i, xs.at[i], 0)

    exchange(lambda k: xs.at[wrap(f + k)], lambda k: strip_of(x.at[0], wrap(f + k)), relay_in, a2a_s, a2a_r, make_in)
    x[0, pl.ds(N_STRIP * strip, strip), :] = x[0, pl.ds(0, strip), :]

    mine = pl.multiple_of(core * half_rows, 16)
    theirs = pl.multiple_of((1 - core) * half_rows, 16)

    def my_rows(u):
        return pl.ds(pl.multiple_of(core * half_rows + u * piece, 16), piece)

    def gram_strip(cur, q):
        left = x[cur, pl.ds(pl.multiple_of(q * strip, strip), strip), :]
        right = x[cur, pl.ds(pl.multiple_of(q * strip, strip), 2 * strip), :]
        both = lax.dot_general(left, right, NT, preferred_element_type=F32)
        for j in range(3):
            a = slice(j * sub3, (j + 1) * sub3)
            j1 = (j + 1) % 3
            part[q, 0:sub3, a] = both[a, a]
            part[q, sub3:2 * sub3, a] = both[a, j1 * sub3:(j1 + 1) * sub3]
        part[q, pl.ds(2 * sub3, strip), :] = both[:, strip:]
        p, hh = q % 2, q // 2
        left = x[cur, pl.ds(pl.multiple_of(p * strip + hh * h, h), h), :]
        right = x[cur, pl.ds(pl.multiple_of((p + 2) * strip, strip), strip), :]
        part[q, pl.ds(2 * sub3 + strip, h), :] = lax.dot_general(left, right, NT, preferred_element_type=F32)

    def unpack():
        for q in range(N_STRIP):
            r = q * strip
            for j in range(3):
                j1 = (j + 1) % 3
                a = pl.ds(r + j * sub3, sub3)
                b = pl.ds(r + j1 * sub3, sub3)
                gram[a, a] = packed[q, pl.ds(0, sub3), pl.ds(j * sub3, sub3)]
                off = packed[q, pl.ds(sub3, sub3), pl.ds(j * sub3, sub3)]
                gram[a, b] = off
                gram[b, a] = off.T
            n = ((q + 1) % N_STRIP) * strip
            off = packed[q, pl.ds(2 * sub3, strip), :]
            gram[pl.ds(r, strip), pl.ds(n, strip)] = off
            gram[pl.ds(n, strip), pl.ds(r, strip)] = off.T
        for p in range(2):
            top = packed[p, pl.ds(2 * sub3 + strip, h), :]
            low = packed[p + 2, pl.ds(2 * sub3 + strip, h), :]
            off = jnp.concatenate([top, low], axis=0)
            gram[pl.ds(p * strip, strip), pl.ds((p + 2) * strip, strip)] = off
            gram[pl.ds((p + 2) * strip, strip), pl.ds(p * strip, strip)] = off.T

    n_tile = cols // 2
    m_tile = N_STRIP * strip // 2

    @pl.loop(0, NS_STEPS)
    def _(it):
        cur = it % 2
        nxt = 1 - cur

        pairs = {}

        def do_gram(j, off):
            q = wrap(chip + off)
            gram_strip(cur, q)
            pairs[j] = send(part.at[q, pl.ds(theirs, half_rows)], pair.at[q], pair_s.at[j], pair_r.at[j], partner)

        rs = {}

        def rs_send(t):
            q = wrap(chip - hop * (t + 1))
            for u in range(N_SUB):
                rows = my_rows(u)
                val = part[q, rows, :] + pair[q, pl.ds(u * piece, piece), :]
                if t > 0:
                    rs[t - 1, u].wait_recv()
                    val = val + ring[t - 1, pl.ds(u * piece, piece), :]
                part[q, rows, :] = val
                rs[t, u] = send(part.at[q, rows], ring.at[t, pl.ds(u * piece, piece)], rs_s.at[t, u], rs_r.at[t, u], ahead)

        do_gram(0, -1)
        do_gram(1, 1)
        pairs[0].wait_recv()
        pairs[1].wait_recv()
        rs_send(0)
        do_gram(2, 2)
        do_gram(3, 0)
        pairs[2].wait_recv()
        rs_send(1)
        rs_send(2)
        pairs[3].wait_recv()

        ag, pg = {}, {}

        def ag_send(t, u):
            q = wrap(chip - hop * t)
            piece_ref = packed.at[q, my_rows(u)]
            if t < N_STRIP - 1:
                ag[t, u] = send(piece_ref, piece_ref, ag_s.at[t, u], ag_r.at[t, u], ahead)
            pg[t, u] = send(piece_ref, piece_ref, pg_s.at[t, u], pg_r.at[t, u], partner)

        for u in range(N_SUB):
            rows = my_rows(u)
            val = part[chip, rows, :] + pair[chip, pl.ds(u * piece, piece), :]
            rs[2, u].wait_recv()
            packed[chip, rows, :] = (val + ring[2, pl.ds(u * piece, piece), :]).astype(BF16)
            ag_send(0, u)
        for t in range(1, N_STRIP):
            for u in range(N_SUB):
                ag[t - 1, u].wait_recv()
                ag_send(t, u)
        for j in range(4):
            pairs[j].wait_send()
        for c in list(rs.values()) + list(ag.values()):
            c.wait_send()
        for c in pg.values():
            c.wait()
        unpack()

        poly_copies = []
        for k in range(2):
            rows = pl.ds(pl.multiple_of((2 * core + k) * strip, strip), strip)
            lhs = gram[rows, :]
            for n in range(2):
                nc = pl.ds(n * m_tile, m_tile)
                sq = jnp.dot(lhs, gram[:, nc], preferred_element_type=F32).astype(BF16)
                poly[rows, nc] = (COEF_B * gram[rows, nc].astype(F32) + COEF_C * sq.astype(F32)).astype(BF16)
            poly_copies.append(send(poly.at[rows], poly.at[rows], poly_s.at[k], poly_r.at[k], partner))

        def apply_poly(i):
            rows = pl.ds(pl.multiple_of(i * strip, strip), strip)
            lhs = poly[rows, :]
            for n in range(2):
                nc = pl.ds(n * n_tile, n_tile)
                px = jnp.dot(lhs, x[cur, pl.ds(0, N_STRIP * strip), nc], preferred_element_type=F32)
                new = (COEF_A * x[cur, rows, nc].astype(F32) + px).astype(BF16)
                x[nxt, rows, nc] = new

                @pl.when(i == 0)
                def _():
                    x[nxt, pl.ds(N_STRIP * strip, strip), nc] = new

        @pl.loop(0, 2)
        def _(k):
            apply_poly(2 * core + k)

        for c in poly_copies:
            c.wait()

        @pl.loop(0, 2)
        def _(k):
            apply_poly(2 * (1 - core) + k)

    last = NS_STEPS % 2
    own = pltpu.make_async_copy(strip_of(x.at[last], f), out_hbm.at[f], own_sem)

    def make_out(k):
        if k == 0:
            own.start()

    exchange(lambda k: strip_of(x.at[last], wrap(f + k)), lambda k: out_hbm.at[wrap(f + k)], relay_out, ret_s, ret_r, make_out)
    own.wait()


def orthogonalize(sq, x0):
    n_mat, strip, cols = x0.shape
    rows = N_STRIP * strip
    packed_rows = 2 * (strip // 3) + strip + strip // 2
    half_rows = packed_rows // 2
    dma = pltpu.SemaphoreType.DMA
    return pl.pallas_call(
        functools.partial(muon_kernel, strip, cols),
        out_shape=jax.ShapeDtypeStruct((n_mat, strip, cols), BF16),
        in_specs=[pl.BlockSpec(memory_space=pltpu.VMEM), pl.BlockSpec(memory_space=pl.ANY)],
        out_specs=pl.BlockSpec(memory_space=pl.ANY),
        scratch_shapes=[
            pltpu.VMEM((N_STRIP, strip, cols), F32),
            pltpu.VMEM((N_STRIP, strip, cols), BF16),
            pltpu.VMEM((2, strip // 2, cols), BF16),
            pltpu.VMEM((2, strip // 2, cols), BF16),
            pltpu.VMEM((2, rows + strip, cols), BF16),
            pltpu.VMEM((N_STRIP, packed_rows, strip), F32),
            pltpu.VMEM((N_STRIP, half_rows, strip), F32),
            pltpu.VMEM((N_STRIP - 1, half_rows, strip), F32),
            pltpu.VMEM((N_STRIP, packed_rows, strip), BF16),
            pltpu.VMEM((rows, rows), BF16),
            pltpu.VMEM((rows, rows), BF16),
            pltpu.VMEM((N_STRIP,) + sq.shape, F32),
            pltpu.VMEM((N_STRIP,) + sq.shape, F32),
            pltpu.VMEM((2,) + sq.shape, F32),
            pltpu.VMEM(sq.shape, F32),
            dma((N_STRIP,)), dma, dma((7,)), dma((7,)), dma((6,)), dma((6,)), dma((6,)), dma((6,)),
            dma((4,)), dma((4,)), dma((3, N_SUB)), dma((3, N_SUB)), dma((3, N_SUB)), dma((3, N_SUB)),
            dma((4, N_SUB)), dma((4, N_SUB)), dma((2,)), dma((2,)),
        ],
        compiler_params=pltpu.CompilerParams(collective_id=0, has_side_effects=True, vmem_limit_bytes=62 * 1024 * 1024),
        name='muon_ns',
    )(sq, x0)


def solution(mesh):
    block_spec = P('stage', 'fsdp', 'tp')
    scalar_spec = P()
    assert mesh.shape['fsdp'] == N_STRIP and mesh.shape['tp'] == 2 * N_STRIP

    def muon_step(weight, momentum, gradient, learn_rate, momentum_coef, weight_decay):
        n_cols = weight.shape[2]

        def local_step(w_blk, m_blk, g_blk, rate_val, coef_val, decay_val):
            g_wide = g_blk.astype(F32)
            m_new = coef_val * m_blk + g_wide
            x_init = g_wide + coef_val * m_new
            sq = jnp.sum(x_init * x_init, axis=(1, 2))
            sq = jnp.broadcast_to(jnp.concatenate([sq, sq])[:, None], (2 * N_STRIP, 128))
            x_home = orthogonalize(sq, x_init)
            step_scale = rate_val * 0.2 * math.sqrt(n_cols)
            keep_scale = 1.0 - rate_val * decay_val
            w_new = keep_scale * w_blk - step_scale * x_home.astype(F32)
            return w_new, m_new

        sharded = jax.shard_map(local_step, mesh=mesh, in_specs=(block_spec, block_spec, block_spec, scalar_spec, scalar_spec, scalar_spec), out_specs=(block_spec, block_spec), check_vma=False)
        return sharded(weight, momentum, gradient, learn_rate, momentum_coef, weight_decay)

    return muon_step
```

```python
import functools
import math

import jax
import jax.numpy as jnp
from jax import lax
from jax.experimental import pallas as pl
from jax.experimental.pallas import tpu as pltpu
from jax.sharding import PartitionSpec as P

NS_STEPS = 5
COEF_A = 3.4445
COEF_B = -4.7750
COEF_C = 2.0315
EPSILON = 1e-7
F32 = jnp.float32
BF16 = jnp.bfloat16
MESH = pl.DeviceIdType.MESH
N_STRIP = 4
N_PIECE = 4
NT = (((1,), (1,)), ((), ()))


def piece_lens(strip):
    last = (2 * (strip // 3) + 3 * strip) // (2 * N_STRIP)
    low = last // 32 * 16
    return [(4 * (strip // 3) + strip) // (2 * N_STRIP), (2 * (strip // 3) + 2 * strip) // (2 * N_STRIP), last - low, low]


def muon_kernel(strip, cols, sq_ref, x0_hbm, out_hbm,
                x0, xs, relay_in, relay_out, x, part, pair, ring, packed, gram, poly, nrm_y, nrm_x, nrm_c, nrm,
                x0_sem, own_sem, nrm_s, nrm_r, a2a_s, a2a_r, ret_s, ret_r,
                pair_s, pair_r, s1_s, s1_r, s2_s, s2_r, g1_s, g1_r, g2_s, g2_r, pg_s, pg_r, poly_s, poly_r):
    f = lax.axis_index('fsdp')
    tp = lax.axis_index('tp')
    chip, core = tp // 2, tp % 2
    sub3 = strip // 3

    def wrap(i):
        return lax.rem(i + 2 * N_STRIP, N_STRIP)

    def y_dev(k):
        return {'fsdp': wrap(f + k)}

    def x_dev(k):
        return {'tp': 2 * wrap(chip + k) + core}

    partner = {'tp': 2 * chip + (1 - core)}
    up, down = x_dev(1), x_dev(-1)

    def copy_to(src, dst, s_sem, r_sem, dev):
        return pltpu.make_async_remote_copy(src_ref=src, dst_ref=dst, send_sem=s_sem, recv_sem=r_sem,
                                            device_id=dev, device_id_type=MESH)

    def send(src, dst, s_sem, r_sem, dev):
        copy = copy_to(src, dst, s_sem, r_sem, dev)
        copy.start()
        return copy

    loads = [pltpu.make_async_copy(x0_hbm.at[i], x0.at[i], x0_sem.at[i]) for i in range(N_STRIP)]
    for c in loads:
        c.start()

    barrier = pltpu.get_barrier_semaphore()
    for dev in [y_dev(1), y_dev(2), y_dev(3), x_dev(1), x_dev(2), x_dev(3), partner]:
        pl.semaphore_signal(barrier, inc=1, device_id=dev, device_id_type=MESH)
    pl.semaphore_wait(barrier, 7)

    nrm_y[f] = sq_ref[...]
    cs = [send(sq_ref, nrm_y.at[f], nrm_s.at[k - 1], nrm_r.at[k - 1], y_dev(k)) for k in (1, 2, 3)]
    for c in cs:
        c.wait()
    nrm_x[chip] = (nrm_y[0] + nrm_y[1]) + (nrm_y[2] + nrm_y[3])
    cs = [send(nrm_x.at[chip], nrm_x.at[chip], nrm_s.at[k + 2], nrm_r.at[k + 2], x_dev(k)) for k in (1, 2, 3)]
    for c in cs:
        c.wait()
    nrm_c[core] = (nrm_x[0] + nrm_x[1]) + (nrm_x[2] + nrm_x[3])
    send(nrm_c.at[core], nrm_c.at[core], nrm_s.at[6], nrm_r.at[6], partner).wait()
    nrm[...] = 1.0 / (jnp.sqrt(nrm_c[0] + nrm_c[1]) + EPSILON)
    for c in loads:
        c.wait()

    tile = strip // 6
    h = strip // 2

    def scale_to(i, dst, base):
        inv = nrm[pl.ds(i, 1), :][:, 0:1]

        @pl.loop(0, strip // tile)
        def _(r):
            rows = pl.ds(pl.multiple_of(r * tile, tile), tile)
            dst[pl.ds(pl.multiple_of(base + r * tile, tile), tile), :] = (x0[i, rows, :] * inv).astype(BF16)

    def exchange(src, dst, relay, s_sem, r_sem, make):
        make(2)
        r0 = send(src(2).at[pl.ds(0, h)], relay.at[0], s_sem.at[0], r_sem.at[0], y_dev(1))
        r1 = send(src(2).at[pl.ds(h, h)], relay.at[1], s_sem.at[1], r_sem.at[1], y_dev(-1))
        make(1)
        d0 = send(src(1), dst(0), s_sem.at[2], r_sem.at[2], y_dev(1))
        make(-1)
        d1 = send(src(-1), dst(0), s_sem.at[3], r_sem.at[3], y_dev(-1))
        make(0)
        r0.wait_recv()
        f0 = send(relay.at[0], dst(-1).at[pl.ds(0, h)], s_sem.at[4], r_sem.at[4], y_dev(1))
        r1.wait_recv()
        f1 = send(relay.at[1], dst(1).at[pl.ds(h, h)], s_sem.at[5], r_sem.at[5], y_dev(-1))
        r0.wait_send()
        r1.wait_send()
        for c in (d0, d1, f0, f1):
            c.wait()

    def strip_of(ref, i):
        return ref.at[pl.ds(pl.multiple_of(i * strip, strip), strip)]

    def make_in(k):
        if k == 0:
            scale_to(f, x.at[0], 0)
        else:
            scale_to(wrap(f + k), xs.at[wrap(f + k)], 0)
        return xs.at[wrap(f + k)]

    d0 = send(make_in(1), x.at[0, pl.ds(3 * strip, strip)], a2a_s.at[2], a2a_r.at[2], y_dev(1))
    d1 = send(make_in(-1), x.at[0, pl.ds(strip, strip)], a2a_s.at[3], a2a_r.at[3], y_dev(-1))
    far_x = make_in(2)
    r0 = send(far_x.at[pl.ds(0, h)], relay_in.at[0], a2a_s.at[0], a2a_r.at[0], y_dev(1))
    r1 = send(far_x.at[pl.ds(h, h)], relay_in.at[1], a2a_s.at[1], a2a_r.at[1], y_dev(-1))
    make_in(0)
    f0 = copy_to(relay_in.at[0], x.at[0, pl.ds(2 * strip, h)], a2a_s.at[4], a2a_r.at[4], y_dev(1))
    f1 = copy_to(relay_in.at[1], x.at[0, pl.ds(2 * strip + h, h)], a2a_s.at[5], a2a_r.at[5], y_dev(-1))

    lens = piece_lens(strip)
    bases = [sum(lens[:u]) * 2 * N_STRIP for u in range(N_PIECE)]

    cuts = [(n // 32) * 16 if u == 0 else (n + 16) // 32 * 16 for u, n in enumerate(lens)]
    starts = [sum(lens[:u]) for u in range(N_PIECE)]

    def half_of(u, q, second):
        at0 = bases[u] + (core * N_STRIP + q) * lens[u] + (cuts[u] if second else 0)
        return pl.ds(pl.multiple_of(at0, 16), lens[u] - cuts[u] if second else cuts[u])

    def slot_of(u, second):
        return pl.ds(starts[u] + (cuts[u] if second else 0), lens[u] - cuts[u] if second else cuts[u])

    def rows_of(u, c, q):
        return pl.ds(pl.multiple_of(bases[u] + (c * N_STRIP + q) * lens[u], 16), lens[u])

    def strip_rows(i):
        return pl.ds(pl.multiple_of(i * strip, strip), strip)

    at = {}
    fill = 0
    for blk in [(0, 0), (1, 1), (0, 1), (3, 3), (3, 0), (3, 1), (2, 2), (2, 3), (2, 1), (2, 0)]:
        at[blk] = fill
        fill += 2 * sub3 if blk[0] == blk[1] else strip

    def put(blk, val):
        if blk[0] != blk[1]:
            part[pl.ds(at[blk], strip), :] = val
            return
        for j in range(3):
            a = slice(j * sub3, (j + 1) * sub3)
            j1 = (j + 1) % 3
            part[pl.ds(at[blk], sub3), a] = val[a, a]
            part[pl.ds(at[blk] + sub3, sub3), a] = val[a, j1 * sub3:(j1 + 1) * sub3]

    def gram_blocks(b, i, js):
        left = x[b, pl.ds(i * strip, strip), :]
        right = [x[b, pl.ds(j * strip, strip), :] for j in js]
        right = right[0] if len(js) == 1 else jnp.concatenate(right, axis=0)
        prod = lax.dot_general(left, right, NT, preferred_element_type=F32)
        for n, j in enumerate(js):
            put((i, j), prod[:, n * strip:(n + 1) * strip])

    def unpack(blk):
        i, j = blk
        if i != j:
            off = packed[pl.ds(at[blk], strip), :]
            gram[pl.ds(i * strip, strip), pl.ds(j * strip, strip)] = off
            gram[pl.ds(j * strip, strip), pl.ds(i * strip, strip)] = off.T
            return
        for k in range(3):
            ra = pl.ds(i * strip + k * sub3, sub3)
            rb = pl.ds(i * strip + (k + 1) % 3 * sub3, sub3)
            gram[ra, ra] = packed[pl.ds(at[blk], sub3), pl.ds(k * sub3, sub3)]
            off = packed[pl.ds(at[blk] + sub3, sub3), pl.ds(k * sub3, sub3)]
            gram[ra, rb] = off
            gram[rb, ra] = off.T

    def poly_copy(k, i):
        rows = strip_rows(i)
        return pltpu.make_async_remote_copy(src_ref=poly.at[rows], dst_ref=poly.at[rows], send_sem=poly_s.at[k],
                                            recv_sem=poly_r.at[k], device_id=partner, device_id_type=MESH)

    def make_poly(i):
        rows = strip_rows(i)
        lhs = gram[rows, :]
        m_tile = N_STRIP * strip // 2
        for n in range(2):
            nc = pl.ds(n * m_tile, m_tile)
            sq = jnp.dot(lhs, gram[:, nc], preferred_element_type=F32).astype(BF16)
            poly[rows, nc] = (COEF_B * gram[rows, nc].astype(F32) + COEF_C * sq.astype(F32)).astype(BF16)

    def apply_poly(b, i, tiles=(0, 1)):
        rows = strip_rows(i)
        lhs = poly[rows, :]
        n_tile = cols // 2
        for n in tiles:
            nc = pl.ds(n * n_tile, n_tile)
            px = jnp.dot(lhs, x[b, :, nc], preferred_element_type=F32)
            x[1 - b, rows, nc] = (COEF_A * x[b, rows, nc].astype(F32) + px).astype(BF16)

    @pl.loop(0, NS_STEPS)
    def _(it):
        b = it % 2
        old = 1 - b
        c_up, c_down, c_far = wrap(chip + 1), wrap(chip - 1), wrap(chip + 2)
        pairs, first, second, near, far, pg = {}, {}, {}, {}, {}, {}
        b0 = poly_copy(0, core)
        b1 = poly_copy(1, 3 - core)

        def pair_send(u):
            src = pl.ds(pl.multiple_of(bases[u] + (1 - core) * N_STRIP * lens[u], 16), N_STRIP * lens[u])
            pairs[u] = send(part.at[src], pair.at[src], pair_s.at[u], pair_r.at[u], partner)

        def sum_1(u):
            pairs[u].wait_recv()
            for q in (c_far, c_up, c_down):
                rows = rows_of(u, core, q)
                part[rows, :] = part[rows, :] + pair[rows, :]
            for k, dev in ((0, up), (1, down)):
                first[u, k] = send(part.at[half_of(u, c_far, k)], ring.at[0, slot_of(u, k)], s1_s.at[k, u], s1_r.at[k, u], dev)

        def sum_1b(u):
            second[u, 1] = send(part.at[half_of(u, c_up, 1)], ring.at[1, slot_of(u, 1)], s2_s.at[1, u], s2_r.at[1, u], up)
            second[u, 2] = send(part.at[half_of(u, c_down, 0)], ring.at[2, slot_of(u, 0)], s2_s.at[2, u], s2_r.at[2, u], down)

        def sum_2(u):
            for k, q, dev in ((0, c_up, up), (1, c_down, down)):
                first[u, k].wait_recv()
                rows = half_of(u, q, k)
                part[rows, :] = part[rows, :] + ring[0, slot_of(u, k), :]
                second[u, 3 * k] = send(part.at[rows], ring.at[1 + k, slot_of(u, k)], s2_s.at[3 * k, u], s2_r.at[3 * k, u], dev)

        def gather_1(u):
            rows = rows_of(u, core, chip)
            val = part[rows, :] + pair[rows, :]
            for k in range(4):
                second[u, k].wait_recv()
            slot = pl.ds(starts[u], lens[u])
            packed[rows, :] = (val + (ring[1, slot, :] + ring[2, slot, :])).astype(BF16)
            for k, dev in ((0, up), (1, down)):
                near[u, k] = send(packed.at[rows], packed.at[rows], g1_s.at[k, u], g1_r.at[k, u], dev)
            pg[u, 0] = send(packed.at[rows], packed.at[rows], pg_s.at[0, u], pg_r.at[0, u], partner)

        def gather_2(u):
            for k, q, dev in ((0, c_down, up), (1, c_up, down)):
                near[u, k].wait_recv()
                half = half_of(u, q, k)
                far[u, k] = send(packed.at[half], packed.at[half], g2_s.at[k, u], g2_r.at[k, u], dev)
            for k, q in ((1, c_down), (2, c_up)):
                rows = rows_of(u, core, q)
                pg[u, k] = send(packed.at[rows], packed.at[rows], pg_s.at[k, u], pg_r.at[k, u], partner)

        def gather_3(u):
            far[u, 0].wait_recv()
            far[u, 1].wait_recv()
            rows = rows_of(u, core, c_far)
            pg[u, 3] = send(packed.at[rows], packed.at[rows], pg_s.at[3, u], pg_r.at[3, u], partner)

        def arrived(u):
            for t in range(N_STRIP):
                pg[u, t].wait_recv()

        @pl.when(it > 0)
        def _():
            make_poly(core)
            b0.start()
            make_poly(3 - core)
            b1.start()
            apply_poly(old, core)
            b0.wait_recv()
            apply_poly(old, 1 - core)

        @pl.when(it == 0)
        def _():
            d1.wait_recv()

        gram_blocks(b, 0, [0, 1])
        gram_blocks(b, 1, [1])
        pair_send(0)

        @pl.when(it > 0)
        def _():
            b1.wait_recv()
            apply_poly(old, 3, (0,))

        sum_1(0)
        sum_1b(0)

        @pl.when(it > 0)
        def _():
            apply_poly(old, 3, (1,))

        @pl.when(it == 0)
        def _():
            d0.wait_recv()

        gram_blocks(b, 3, [3, 0, 1])
        pair_send(1)
        sum_2(0)

        @pl.when(it > 0)
        def _():
            apply_poly(old, 2, (0,))

        sum_1(1)
        sum_1b(1)

        @pl.when(it > 0)
        def _():
            apply_poly(old, 2, (1,))
            b0.wait_send()
            b1.wait_send()

        gather_1(0)

        @pl.when(it == 0)
        def _():
            r0.wait_recv()
            f0.start()
            r1.wait_recv()
            f1.start()

        sum_2(1)

        @pl.when(it == 0)
        def _():
            f0.wait_recv()
            f1.wait_recv()

        gram_blocks(b, 2, [2, 3])
        gram_blocks(b, 2, [1, 0])
        pair_send(2)
        pair_send(3)
        gather_2(0)
        sum_1(2)
        sum_1(3)
        sum_1b(2)
        sum_1b(3)
        gather_1(1)
        sum_2(2)
        sum_2(3)
        gather_3(0)
        gather_2(1)
        arrived(0)
        for blk in [(0, 0), (1, 1), (0, 1)]:
            unpack(blk)
        gather_1(2)
        gather_1(3)
        gather_3(1)
        arrived(1)
        for blk in [(3, 3), (3, 0), (3, 1)]:
            unpack(blk)
        gather_2(2)
        gather_2(3)
        gather_3(2)
        gather_3(3)
        arrived(2)
        unpack((2, 2))
        unpack((2, 3))
        arrived(3)
        unpack((2, 1))
        unpack((2, 0))
        for group in (pairs, first, second, near, far, pg):
            for c in group.values():
                c.wait_send()

    for c in (d0, d1, r0, r1, f0, f1):
        c.wait_send()

    last = NS_STEPS % 2
    own = pltpu.make_async_copy(x.at[last, pl.ds(0, strip)], out_hbm.at[f], own_sem)
    b0 = poly_copy(0, 2 - core)
    b1 = poly_copy(1, 3 - 3 * core)
    make_poly(2 - core)
    b0.start()
    make_poly(3 - 3 * core)
    b1.start()
    b0.wait_recv()

    def make_out(k):
        if k == -1:
            b1.wait_recv()
        apply_poly(1 - last, k % N_STRIP)
        if k == 0:
            own.start()

    exchange(lambda k: strip_of(x.at[last], k % N_STRIP), lambda k: out_hbm.at[wrap(f + k)], relay_out, ret_s, ret_r, make_out)
    own.wait()
    b0.wait_send()
    b1.wait_send()


def orthogonalize(sq, x0):
    n_mat, strip, cols = x0.shape
    rows = N_STRIP * strip
    packed_rows = 2 * N_STRIP * sum(piece_lens(strip))
    dma = pltpu.SemaphoreType.DMA
    return pl.pallas_call(
        functools.partial(muon_kernel, strip, cols),
        out_shape=jax.ShapeDtypeStruct((n_mat, strip, cols), BF16),
        in_specs=[pl.BlockSpec(memory_space=pltpu.VMEM), pl.BlockSpec(memory_space=pl.ANY)],
        out_specs=pl.BlockSpec(memory_space=pl.ANY),
        scratch_shapes=[
            pltpu.VMEM((N_STRIP, strip, cols), F32),
            pltpu.VMEM((N_STRIP, strip, cols), BF16),
            pltpu.VMEM((2, strip // 2, cols), BF16),
            pltpu.VMEM((2, strip // 2, cols), BF16),
            pltpu.VMEM((2, rows, cols), BF16),
            pltpu.VMEM((packed_rows, strip), F32),
            pltpu.VMEM((packed_rows, strip), F32),
            pltpu.VMEM((N_STRIP - 1, packed_rows // 8, strip), F32),
            pltpu.VMEM((packed_rows, strip), BF16),
            pltpu.VMEM((rows, rows), BF16),
            pltpu.VMEM((rows, rows), BF16),
            pltpu.VMEM((N_STRIP,) + sq.shape, F32),
            pltpu.VMEM((N_STRIP,) + sq.shape, F32),
            pltpu.VMEM((2,) + sq.shape, F32),
            pltpu.VMEM(sq.shape, F32),
            dma((N_STRIP,)), dma, dma((7,)), dma((7,)), dma((6,)), dma((6,)), dma((6,)), dma((6,)),
            dma((N_PIECE,)), dma((N_PIECE,)), dma((2, N_PIECE)), dma((2, N_PIECE)), dma((4, N_PIECE)), dma((4, N_PIECE)),
            dma((2, N_PIECE)), dma((2, N_PIECE)), dma((2, N_PIECE)), dma((2, N_PIECE)),
            dma((4, N_PIECE)), dma((4, N_PIECE)), dma((2,)), dma((2,)),
        ],
        compiler_params=pltpu.CompilerParams(collective_id=0, has_side_effects=True, vmem_limit_bytes=62 * 1024 * 1024),
        name='muon_ns',
    )(sq, x0)


def solution(mesh):
    block_spec = P('stage', 'fsdp', 'tp')
    scalar_spec = P()
    assert mesh.shape['fsdp'] == N_STRIP and mesh.shape['tp'] == 2 * N_STRIP

    def muon_step(weight, momentum, gradient, learn_rate, momentum_coef, weight_decay):
        n_cols = weight.shape[2]

        def local_step(w_blk, m_blk, g_blk, rate_val, coef_val, decay_val):
            g_wide = g_blk.astype(F32)
            m_new = coef_val * m_blk + g_wide
            x_init = g_wide + coef_val * m_new
            sq = jnp.sum(x_init * x_init, axis=(1, 2))
            sq = jnp.broadcast_to(jnp.concatenate([sq, sq])[:, None], (2 * N_STRIP, 128))
            x_home = orthogonalize(sq, x_init)
            step_scale = rate_val * 0.2 * math.sqrt(n_cols)
            keep_scale = 1.0 - rate_val * decay_val
            w_new = keep_scale * w_blk - step_scale * x_home.astype(F32)
            return w_new, m_new

        sharded = jax.shard_map(local_step, mesh=mesh, in_specs=(block_spec, block_spec, block_spec, scalar_spec, scalar_spec, scalar_spec), out_specs=(block_spec, block_spec), check_vma=False)
        return sharded(weight, momentum, gradient, learn_rate, momentum_coef, weight_decay)

    return muon_step
```

```python
import functools
import math

import jax
import jax.numpy as jnp
from jax import lax
from jax.experimental import pallas as pl
from jax.experimental.pallas import tpu as pltpu
from jax.sharding import PartitionSpec as P

NS_STEPS = 5
COEF_A = 3.4445
COEF_B = -4.7750
COEF_C = 2.0315
EPSILON = 1e-7
F32 = jnp.float32
BF16 = jnp.bfloat16
MESH = pl.DeviceIdType.MESH
N_STRIP = 4
N_PIECE = 4
NT = (((1,), (1,)), ((), ()))


def piece_lens(strip):
    last = (2 * (strip // 3) + 3 * strip) // (2 * N_STRIP)
    low = last // 32 * 16
    return [(4 * (strip // 3) + strip) // (2 * N_STRIP), (2 * (strip // 3) + 2 * strip) // (2 * N_STRIP), last - low, low]


def muon_kernel(strip, cols, sq_ref, x0_hbm, out_hbm,
                x0, xs, relay_in, relay_out, x, part, pair, ring, packed, gram, poly, nrm_y, nrm_x, nrm_c, nrm,
                x0_sem, own_sem, nrm_s, nrm_r, a2a_s, a2a_r, ret_s, ret_r,
                pair_s, pair_r, s1_s, s1_r, s2_s, s2_r, g1_s, g1_r, g2_s, g2_r, pg_s, pg_r, poly_s, poly_r):
    f = lax.axis_index('fsdp')
    tp = lax.axis_index('tp')
    chip, core = tp // 2, tp % 2
    sub3 = strip // 3

    def wrap(i):
        return lax.rem(i + 2 * N_STRIP, N_STRIP)

    def y_dev(k):
        return {'fsdp': wrap(f + k)}

    def x_dev(k):
        return {'tp': 2 * wrap(chip + k) + core}

    partner = {'tp': 2 * chip + (1 - core)}
    up, down = x_dev(1), x_dev(-1)

    def copy_to(src, dst, s_sem, r_sem, dev):
        return pltpu.make_async_remote_copy(src_ref=src, dst_ref=dst, send_sem=s_sem, recv_sem=r_sem,
                                            device_id=dev, device_id_type=MESH)

    def send(src, dst, s_sem, r_sem, dev):
        copy = copy_to(src, dst, s_sem, r_sem, dev)
        copy.start()
        return copy

    loads = [pltpu.make_async_copy(x0_hbm.at[i], x0.at[i], x0_sem.at[i]) for i in range(N_STRIP)]
    for c in loads:
        c.start()

    barrier = pltpu.get_barrier_semaphore()
    for dev in [y_dev(1), y_dev(2), y_dev(3), x_dev(1), x_dev(2), x_dev(3), partner]:
        pl.semaphore_signal(barrier, inc=1, device_id=dev, device_id_type=MESH)
    pl.semaphore_wait(barrier, 7)

    nrm_y[f] = sq_ref[...]
    cs = [send(sq_ref, nrm_y.at[f], nrm_s.at[k - 1], nrm_r.at[k - 1], y_dev(k)) for k in (1, 2, 3)]
    for c in cs:
        c.wait()
    nrm_x[chip] = (nrm_y[0] + nrm_y[1]) + (nrm_y[2] + nrm_y[3])
    cs = [send(nrm_x.at[chip], nrm_x.at[chip], nrm_s.at[k + 2], nrm_r.at[k + 2], x_dev(k)) for k in (1, 2, 3)]
    for c in cs:
        c.wait()
    nrm_c[core] = (nrm_x[0] + nrm_x[1]) + (nrm_x[2] + nrm_x[3])
    send(nrm_c.at[core], nrm_c.at[core], nrm_s.at[6], nrm_r.at[6], partner).wait()
    nrm[...] = 1.0 / (jnp.sqrt(nrm_c[0] + nrm_c[1]) + EPSILON)
    for c in loads:
        c.wait()

    tile = strip // 6
    h = strip // 2

    def scale_to(i, dst, base):
        inv = nrm[pl.ds(i, 1), :][:, 0:1]

        @pl.loop(0, strip // tile)
        def _(r):
            rows = pl.ds(pl.multiple_of(r * tile, tile), tile)
            dst[pl.ds(pl.multiple_of(base + r * tile, tile), tile), :] = (x0[i, rows, :] * inv).astype(BF16)

    def exchange(src, dst, relay, s_sem, r_sem, make):
        make(2)
        r0 = send(src(2).at[pl.ds(0, h)], relay.at[0], s_sem.at[0], r_sem.at[0], y_dev(1))
        r1 = send(src(2).at[pl.ds(h, h)], relay.at[1], s_sem.at[1], r_sem.at[1], y_dev(-1))
        make(1)
        d0 = send(src(1), dst(0), s_sem.at[2], r_sem.at[2], y_dev(1))
        make(-1)
        d1 = send(src(-1), dst(0), s_sem.at[3], r_sem.at[3], y_dev(-1))
        make(0)
        r0.wait_recv()
        f0 = send(relay.at[0], dst(-1).at[pl.ds(0, h)], s_sem.at[4], r_sem.at[4], y_dev(1))
        r1.wait_recv()
        f1 = send(relay.at[1], dst(1).at[pl.ds(h, h)], s_sem.at[5], r_sem.at[5], y_dev(-1))
        r0.wait_send()
        r1.wait_send()
        for c in (d0, d1, f0, f1):
            c.wait()

    def strip_of(ref, i):
        return ref.at[pl.ds(pl.multiple_of(i * strip, strip), strip)]

    def make_in(k):
        if k == 0:
            scale_to(f, x.at[0], 0)
        else:
            scale_to(wrap(f + k), xs.at[wrap(f + k)], 0)
        return xs.at[wrap(f + k)]

    d0 = send(make_in(1), x.at[0, pl.ds(3 * strip, strip)], a2a_s.at[2], a2a_r.at[2], y_dev(1))
    d1 = send(make_in(-1), x.at[0, pl.ds(strip, strip)], a2a_s.at[3], a2a_r.at[3], y_dev(-1))
    far_x = make_in(2)
    r0 = send(far_x.at[pl.ds(0, h)], relay_in.at[0], a2a_s.at[0], a2a_r.at[0], y_dev(1))
    r1 = send(far_x.at[pl.ds(h, h)], relay_in.at[1], a2a_s.at[1], a2a_r.at[1], y_dev(-1))
    make_in(0)
    f0 = copy_to(relay_in.at[0], x.at[0, pl.ds(2 * strip, h)], a2a_s.at[4], a2a_r.at[4], y_dev(1))
    f1 = copy_to(relay_in.at[1], x.at[0, pl.ds(2 * strip + h, h)], a2a_s.at[5], a2a_r.at[5], y_dev(-1))

    lens = piece_lens(strip)
    bases = [sum(lens[:u]) * 2 * N_STRIP for u in range(N_PIECE)]

    cuts = [(n // 32) * 16 if u == 0 else (n + 16) // 32 * 16 for u, n in enumerate(lens)]
    starts = [sum(lens[:u]) for u in range(N_PIECE)]

    def half_of(u, q, second):
        at0 = bases[u] + (core * N_STRIP + q) * lens[u] + (cuts[u] if second else 0)
        return pl.ds(pl.multiple_of(at0, 16), lens[u] - cuts[u] if second else cuts[u])

    def slot_of(u, second):
        return pl.ds(starts[u] + (cuts[u] if second else 0), lens[u] - cuts[u] if second else cuts[u])

    def rows_of(u, c, q):
        return pl.ds(pl.multiple_of(bases[u] + (c * N_STRIP + q) * lens[u], 16), lens[u])

    def strip_rows(i):
        return pl.ds(pl.multiple_of(i * strip, strip), strip)

    at = {}
    fill = 0
    for blk in [(0, 0), (1, 1), (0, 1), (3, 3), (3, 0), (3, 1), (2, 2), (2, 3), (2, 1), (2, 0)]:
        at[blk] = fill
        fill += 2 * sub3 if blk[0] == blk[1] else strip

    def put(blk, val):
        if blk[0] != blk[1]:
            part[pl.ds(at[blk], strip), :] = val
            return
        for j in range(3):
            a = slice(j * sub3, (j + 1) * sub3)
            j1 = (j + 1) % 3
            part[pl.ds(at[blk], sub3), a] = val[a, a]
            part[pl.ds(at[blk] + sub3, sub3), a] = val[a, j1 * sub3:(j1 + 1) * sub3]

    def gram_blocks(b, i, js):
        left = x[b, pl.ds(i * strip, strip), :]
        right = [x[b, pl.ds(j * strip, strip), :] for j in js]
        right = right[0] if len(js) == 1 else jnp.concatenate(right, axis=0)
        prod = lax.dot_general(left, right, NT, preferred_element_type=F32)
        for n, j in enumerate(js):
            put((i, j), prod[:, n * strip:(n + 1) * strip])

    def unpack(blk):
        i, j = blk
        if i != j:
            off = packed[pl.ds(at[blk], strip), :]
            gram[pl.ds(i * strip, strip), pl.ds(j * strip, strip)] = off
            gram[pl.ds(j * strip, strip), pl.ds(i * strip, strip)] = off.T
            return
        for k in range(3):
            ra = pl.ds(i * strip + k * sub3, sub3)
            rb = pl.ds(i * strip + (k + 1) % 3 * sub3, sub3)
            gram[ra, ra] = packed[pl.ds(at[blk], sub3), pl.ds(k * sub3, sub3)]
            off = packed[pl.ds(at[blk] + sub3, sub3), pl.ds(k * sub3, sub3)]
            gram[ra, rb] = off
            gram[rb, ra] = off.T

    def poly_copy(k, i):
        rows = strip_rows(i)
        return pltpu.make_async_remote_copy(src_ref=poly.at[rows], dst_ref=poly.at[rows], send_sem=poly_s.at[k],
                                            recv_sem=poly_r.at[k], device_id=partner, device_id_type=MESH)

    def make_poly(i):
        rows = strip_rows(i)
        lhs = gram[rows, :]
        m_tile = N_STRIP * strip // 2
        for n in range(2):
            nc = pl.ds(n * m_tile, m_tile)
            sq = jnp.dot(lhs, gram[:, nc], preferred_element_type=F32).astype(BF16)
            poly[rows, nc] = (COEF_B * gram[rows, nc].astype(F32) + COEF_C * sq.astype(F32)).astype(BF16)

    def apply_poly(b, i, tiles=(0, 1)):
        rows = strip_rows(i)
        lhs = poly[rows, :]
        n_tile = cols // 2
        for n in tiles:
            nc = pl.ds(n * n_tile, n_tile)
            px = jnp.dot(lhs, x[b, :, nc], preferred_element_type=F32)
            x[1 - b, rows, nc] = (COEF_A * x[b, rows, nc].astype(F32) + px).astype(BF16)

    @pl.loop(0, NS_STEPS)
    def _(it):
        b = it % 2
        old = 1 - b
        c_up, c_down, c_far = wrap(chip + 1), wrap(chip - 1), wrap(chip + 2)
        pairs, first, second, near, far, pg = {}, {}, {}, {}, {}, {}
        b0 = poly_copy(0, core)
        b1 = poly_copy(1, 3 - core)

        def pair_send(u):
            src = pl.ds(pl.multiple_of(bases[u] + (1 - core) * N_STRIP * lens[u], 16), N_STRIP * lens[u])
            pairs[u] = send(part.at[src], pair.at[src], pair_s.at[u], pair_r.at[u], partner)

        def sum_1(u):
            pairs[u].wait_recv()
            for q in (c_far, c_up, c_down):
                rows = rows_of(u, core, q)
                part[rows, :] = part[rows, :] + pair[rows, :]
            for k, dev in ((0, up), (1, down)):
                first[u, k] = send(part.at[half_of(u, c_far, k)], ring.at[0, slot_of(u, k)], s1_s.at[k, u], s1_r.at[k, u], dev)

        def sum_1b(u):
            second[u, 1] = send(part.at[half_of(u, c_up, 1)], ring.at[1, slot_of(u, 1)], s2_s.at[1, u], s2_r.at[1, u], up)
            second[u, 2] = send(part.at[half_of(u, c_down, 0)], ring.at[2, slot_of(u, 0)], s2_s.at[2, u], s2_r.at[2, u], down)

        def sum_2(u):
            for k, q, dev in ((0, c_up, up), (1, c_down, down)):
                first[u, k].wait_recv()
                rows = half_of(u, q, k)
                part[rows, :] = part[rows, :] + ring[0, slot_of(u, k), :]
                second[u, 3 * k] = send(part.at[rows], ring.at[1 + k, slot_of(u, k)], s2_s.at[3 * k, u], s2_r.at[3 * k, u], dev)

        def gather_1(u):
            rows = rows_of(u, core, chip)
            val = part[rows, :] + pair[rows, :]
            for k in range(4):
                second[u, k].wait_recv()
            slot = pl.ds(starts[u], lens[u])
            packed[rows, :] = (val + (ring[1, slot, :] + ring[2, slot, :])).astype(BF16)
            for k, dev in ((0, up), (1, down)):
                near[u, k] = send(packed.at[rows], packed.at[rows], g1_s.at[k, u], g1_r.at[k, u], dev)
            pg[u, 0] = send(packed.at[rows], packed.at[rows], pg_s.at[0, u], pg_r.at[0, u], partner)

        def gather_2(u):
            for k, q, dev in ((0, c_down, up), (1, c_up, down)):
                near[u, k].wait_recv()
                half = half_of(u, q, k)
                far[u, k] = send(packed.at[half], packed.at[half], g2_s.at[k, u], g2_r.at[k, u], dev)
            for k, q in ((1, c_down), (2, c_up)):
                rows = rows_of(u, core, q)
                pg[u, k] = send(packed.at[rows], packed.at[rows], pg_s.at[k, u], pg_r.at[k, u], partner)

        def gather_3(u):
            far[u, 0].wait_recv()
            far[u, 1].wait_recv()
            rows = rows_of(u, core, c_far)
            pg[u, 3] = send(packed.at[rows], packed.at[rows], pg_s.at[3, u], pg_r.at[3, u], partner)

        def arrived(u):
            for t in range(N_STRIP):
                pg[u, t].wait_recv()

        @pl.when(it > 0)
        def _():
            make_poly(core)
            b0.start()
            make_poly(3 - core)
            b1.start()
            apply_poly(old, core)
            b0.wait_recv()
            apply_poly(old, 1 - core)

        @pl.when(it == 0)
        def _():
            d1.wait_recv()

        gram_blocks(b, 0, [0, 1])
        gram_blocks(b, 1, [1])
        pair_send(0)

        @pl.when(it > 0)
        def _():
            b1.wait_recv()
            apply_poly(old, 3, (0,))

        sum_1(0)
        sum_1b(0)

        @pl.when(it > 0)
        def _():
            apply_poly(old, 3, (1,))

        @pl.when(it == 0)
        def _():
            d0.wait_recv()

        gram_blocks(b, 3, [3, 0, 1])
        pair_send(1)

        @pl.when(it > 0)
        def _():
            apply_poly(old, 2, (0,))

        sum_2(0)
        sum_1(1)
        sum_1b(1)

        @pl.when(it > 0)
        def _():
            apply_poly(old, 2, (1,))
            b0.wait_send()
            b1.wait_send()

        gather_1(0)

        @pl.when(it == 0)
        def _():
            r0.wait_recv()
            f0.start()
            r1.wait_recv()
            f1.start()

        sum_2(1)

        @pl.when(it == 0)
        def _():
            f0.wait_recv()
            f1.wait_recv()

        gram_blocks(b, 2, [2, 3])
        gram_blocks(b, 2, [1, 0])
        pair_send(2)
        pair_send(3)
        gather_2(0)
        sum_1(2)
        sum_1(3)
        sum_1b(2)
        sum_1b(3)
        gather_1(1)
        sum_2(2)
        sum_2(3)
        gather_3(0)
        gather_2(1)
        arrived(0)
        for blk in [(0, 0), (1, 1), (0, 1)]:
            unpack(blk)
        gather_1(2)
        gather_1(3)
        gather_3(1)
        arrived(1)
        for blk in [(3, 3), (3, 0), (3, 1)]:
            unpack(blk)
        gather_2(2)
        gather_2(3)
        gather_3(2)
        gather_3(3)
        arrived(2)
        unpack((2, 2))
        unpack((2, 3))
        arrived(3)
        unpack((2, 1))
        unpack((2, 0))
        for group in (pairs, first, second, near, far, pg):
            for c in group.values():
                c.wait_send()

    for c in (d0, d1, r0, r1, f0, f1):
        c.wait_send()

    last = NS_STEPS % 2
    own = pltpu.make_async_copy(x.at[last, pl.ds(0, strip)], out_hbm.at[f], own_sem)
    b0 = poly_copy(0, 2 - core)
    b1 = poly_copy(1, 3 - 3 * core)
    make_poly(2 - core)
    b0.start()
    make_poly(3 - 3 * core)
    b1.start()
    b0.wait_recv()

    def make_out(k):
        if k == -1:
            b1.wait_recv()
        apply_poly(1 - last, k % N_STRIP)
        if k == 0:
            own.start()

    exchange(lambda k: strip_of(x.at[last], k % N_STRIP), lambda k: out_hbm.at[wrap(f + k)], relay_out, ret_s, ret_r, make_out)
    own.wait()
    b0.wait_send()
    b1.wait_send()


def orthogonalize(sq, x0):
    n_mat, strip, cols = x0.shape
    rows = N_STRIP * strip
    packed_rows = 2 * N_STRIP * sum(piece_lens(strip))
    dma = pltpu.SemaphoreType.DMA
    return pl.pallas_call(
        functools.partial(muon_kernel, strip, cols),
        out_shape=jax.ShapeDtypeStruct((n_mat, strip, cols), BF16),
        in_specs=[pl.BlockSpec(memory_space=pltpu.VMEM), pl.BlockSpec(memory_space=pl.ANY)],
        out_specs=pl.BlockSpec(memory_space=pl.ANY),
        scratch_shapes=[
            pltpu.VMEM((N_STRIP, strip, cols), F32),
            pltpu.VMEM((N_STRIP, strip, cols), BF16),
            pltpu.VMEM((2, strip // 2, cols), BF16),
            pltpu.VMEM((2, strip // 2, cols), BF16),
            pltpu.VMEM((2, rows, cols), BF16),
            pltpu.VMEM((packed_rows, strip), F32),
            pltpu.VMEM((packed_rows, strip), F32),
            pltpu.VMEM((N_STRIP - 1, packed_rows // 8, strip), F32),
            pltpu.VMEM((packed_rows, strip), BF16),
            pltpu.VMEM((rows, rows), BF16),
            pltpu.VMEM((rows, rows), BF16),
            pltpu.VMEM((N_STRIP,) + sq.shape, F32),
            pltpu.VMEM((N_STRIP,) + sq.shape, F32),
            pltpu.VMEM((2,) + sq.shape, F32),
            pltpu.VMEM(sq.shape, F32),
            dma((N_STRIP,)), dma, dma((7,)), dma((7,)), dma((6,)), dma((6,)), dma((6,)), dma((6,)),
            dma((N_PIECE,)), dma((N_PIECE,)), dma((2, N_PIECE)), dma((2, N_PIECE)), dma((4, N_PIECE)), dma((4, N_PIECE)),
            dma((2, N_PIECE)), dma((2, N_PIECE)), dma((2, N_PIECE)), dma((2, N_PIECE)),
            dma((4, N_PIECE)), dma((4, N_PIECE)), dma((2,)), dma((2,)),
        ],
        compiler_params=pltpu.CompilerParams(collective_id=0, has_side_effects=True, vmem_limit_bytes=62 * 1024 * 1024),
        name='muon_ns',
    )(sq, x0)


def solution(mesh):
    block_spec = P('stage', 'fsdp', 'tp')
    scalar_spec = P()
    assert mesh.shape['fsdp'] == N_STRIP and mesh.shape['tp'] == 2 * N_STRIP

    def muon_step(weight, momentum, gradient, learn_rate, momentum_coef, weight_decay):
        n_cols = weight.shape[2]

        def local_step(w_blk, m_blk, g_blk, rate_val, coef_val, decay_val):
            g_wide = g_blk.astype(F32)
            m_new = coef_val * m_blk + g_wide
            x_init = g_wide + coef_val * m_new
            sq = jnp.sum(x_init * x_init, axis=(1, 2))
            sq = jnp.broadcast_to(jnp.concatenate([sq, sq])[:, None], (2 * N_STRIP, 128))
            x_home = orthogonalize(sq, x_init)
            step_scale = rate_val * 0.2 * math.sqrt(n_cols)
            keep_scale = 1.0 - rate_val * decay_val
            w_new = keep_scale * w_blk - step_scale * x_home.astype(F32)
            return w_new, m_new

        sharded = jax.shard_map(local_step, mesh=mesh, in_specs=(block_spec, block_spec, block_spec, scalar_spec, scalar_spec, scalar_spec), out_specs=(block_spec, block_spec), check_vma=False)
        return sharded(weight, momentum, gradient, learn_rate, momentum_coef, weight_decay)

    return muon_step
```
